256 devices in a mesh: group: 4 (over y, x), space: 64 (over z, core).
Axes of the slice: x: 2, y: 2, z: 32, core: 2. Of those that a mesh axis runs over, the one named last changes fastest.
The devices are a block of a 4x8x32 slice.
Arguments:
- field: bfloat16 [8, 512, 512, 256], P('group', 'space'), parts along dimension 0, may hold values from -6 to 6
- spectral_weight: bfloat16 [1024, 2, 256, 256], P('space'), may hold values from -5 to 5
- skip_weight: bfloat16 [256, 256], replicated, may hold values from -0.375 to 0.375
Outputs:
- layer_out: bfloat16 [8, 512, 512, 256], P('group', 'space'), parts along dimension 0
The draws below stay inside these ranges and needn't reach their ends.
There are 4 independent parts, one for each index of `group`. The reference program is written for one: setup_inputs(seed, part) draws one part's arguments, and reference() takes and returns one part's arrays. A program takes and returns all parts, laid end to end along the dimension named above; an argument that names none is the same for every part. Nothing has to cross between parts.
All inputs are finite; a program needn't handle non-finite values.
Results may differ from the reference program's by a relative error of at most 0.008.
Values may be sent and summed in bfloat16 or wider, within the bound.
A program may use at most 128 MiB of HBM per device.

```python
import math
import jax
import jax.numpy as jnp
from jax import lax

NX = 512
NY = 512
C = 256
KX = 32
KY = 32
MODES = 1024


def steps_of(rng, dims, cuts, low, largest):
    def one(position, parts):
        heights = jax.random.uniform(jax.random.fold_in(jax.random.fold_in(rng, 6), position), (parts,), jnp.float32, low / len(cuts), largest / len(cuts))
        return jnp.repeat(jnp.exp(heights), dims[position] // parts).reshape((-1,) + (1,) * (len(dims) - position - 1))

    factor_of = one(*cuts[0])
    for cut in cuts[1:]:
        factor_of = factor_of * one(*cut)
    return factor_of


def gaussian(key, shape, spread, most, shards=(), held_as=jnp.bfloat16):
    factor_of = steps_of(key, shape, shards, -0.22, 0.18) if shards else 1.0
    entries = jax.random.normal(key, shape, jnp.float32) * spread * factor_of
    return jnp.minimum(jnp.maximum(entries, -most), most).astype(held_as)


def setup_inputs(seed: int = 0, part: int = 0) -> dict:
    key_of = jax.random.split(jax.random.key(seed), 4)
    part_splits = jax.random.split(jax.random.fold_in(key_of[3], part), 4)
    return {
        "field": gaussian(part_splits[0], (2, NX, NY, C), 1.0, 6.0, ((1, 64),)),
        "spectral_weight": gaussian(key_of[1], (MODES, 2, C, C), (11.0 * C ** -0.5), 5.0, ((0, 64),)),
        "skip_weight": gaussian(key_of[2], (C, C), C ** -0.5, 0.375),
    }


def wave_table(kept_index, positions, length, kept, sign):
    frequency = jnp.where(kept_index < kept // 2, kept_index, length - kept + kept_index)
    phase = (frequency[:, None] * positions[None, :]) % length
    angle = (2.0 * math.pi / length) * phase.astype(jnp.float32)
    factor = length ** -0.5
    return jnp.cos(angle) * factor, sign * jnp.sin(angle) * factor


def rounded(values):
    return lax.optimization_barrier(values.astype(jnp.bfloat16)).astype(jnp.float32)


def reference(field, spectral_weight, skip_weight):
    highest = lax.Precision.HIGHEST
    fy_re, fy_im = wave_table(jnp.arange(KY, dtype=jnp.int32), jnp.arange(NY, dtype=jnp.int32), NY, KY, -1.0)
    fy_re = rounded(fy_re)
    fy_im = rounded(fy_im)
    skip_full = skip_weight.astype(jnp.float32)
    field_blocks = field.reshape(2, NX // 8, 8, NY, C).transpose(1, 0, 2, 3, 4)

    def forward_rows(block):
        values = block.astype(jnp.float32)
        real_part = jnp.einsum('ky,xyc->xkc', fy_re, values[0], precision=highest) - jnp.einsum('ky,xyc->xkc', fy_im, values[1], precision=highest)
        imag_part = jnp.einsum('ky,xyc->xkc', fy_re, values[1], precision=highest) + jnp.einsum('ky,xyc->xkc', fy_im, values[0], precision=highest)
        return jnp.stack([real_part, imag_part])

    yspec = lax.map(forward_rows, field_blocks).transpose(1, 0, 2, 3, 4).reshape(2, NX, KY, C)
    fx_re, fx_im = wave_table(jnp.arange(KX, dtype=jnp.int32), jnp.arange(NX, dtype=jnp.int32), NX, KX, -1.0)
    spec_re = jnp.einsum('kx,xyc->kyc', fx_re, yspec[0], precision=highest) - jnp.einsum('kx,xyc->kyc', fx_im, yspec[1], precision=highest)
    spec_im = jnp.einsum('kx,xyc->kyc', fx_re, yspec[1], precision=highest) + jnp.einsum('kx,xyc->kyc', fx_im, yspec[0], precision=highest)
    spec = jnp.stack([spec_re, spec_im], axis=2).reshape(KX * KY, 2, C).astype(jnp.bfloat16)
    product = jnp.einsum('mrc,mwco->mrwo', spec.astype(jnp.float32), spectral_weight.astype(jnp.float32), precision=highest)
    mixed = jnp.stack([product[:, 0, 0] - product[:, 1, 1], product[:, 0, 1] + product[:, 1, 0]], axis=1).astype(jnp.bfloat16)
    gx_re, gx_im = wave_table(jnp.arange(KX, dtype=jnp.int32), jnp.arange(NX, dtype=jnp.int32), NX, KX, 1.0)
    gx_re = rounded(gx_re).T
    gx_im = rounded(gx_im).T
    modes = mixed.astype(jnp.float32).reshape(KX, KY, 2, C)
    zx_re = jnp.einsum('xk,kyc->xyc', gx_re, modes[:, :, 0], precision=highest) - jnp.einsum('xk,kyc->xyc', gx_im, modes[:, :, 1], precision=highest)
    zx_im = jnp.einsum('xk,kyc->xyc', gx_re, modes[:, :, 1], precision=highest) + jnp.einsum('xk,kyc->xyc', gx_im, modes[:, :, 0], precision=highest)
    zx_blocks = jnp.stack([zx_re, zx_im]).reshape(2, NX // 8, 8, KY, C).transpose(1, 0, 2, 3, 4)
    gy_re, gy_im = wave_table(jnp.arange(KY, dtype=jnp.int32), jnp.arange(NY, dtype=jnp.int32), NY, KY, 1.0)
    gy_re = gy_re.T
    gy_im = gy_im.T

    def finish_rows(pair):
        block, zblock = pair
        values = block.astype(jnp.float32)
        out_re = jnp.einsum('yk,xkc->xyc', gy_re, zblock[0], precision=highest) - jnp.einsum('yk,xkc->xyc', gy_im, zblock[1], precision=highest)
        out_im = jnp.einsum('yk,xkc->xyc', gy_re, zblock[1], precision=highest) + jnp.einsum('yk,xkc->xyc', gy_im, zblock[0], precision=highest)
        out_re = out_re + jnp.einsum('xyc,co->xyo', values[0], skip_full, precision=highest)
        out_im = out_im + jnp.einsum('xyc,co->xyo', values[1], skip_full, precision=highest)
        return jnp.stack([out_re, out_im]).astype(jnp.bfloat16)

    result = lax.map(finish_rows, (field_blocks, zx_blocks))
    return result.transpose(1, 0, 2, 3, 4).reshape(2, NX, NY, C)
```

```python
import functools
import math

import jax
import jax.numpy as jnp
import numpy as np
from jax import lax
from jax.experimental import pallas as pl
from jax.experimental.pallas import tpu as pltpu
from jax.sharding import PartitionSpec as P

KX = 32
KY = 32
HALF = KY // 2
CHUNK = 2 * HALF
MESH = pl.DeviceIdType.MESH
F32 = jnp.float32
BF16 = jnp.bfloat16
NEAR = (2, 1, -1)
FAR = (4, 3, -3, 2, -2, 1, -1, 0)


def frequency_of(index, length, kept):
    return np.where(index < kept // 2, index, length - kept + index)


def np_table(kept, length):
    frequency = frequency_of(np.arange(kept), length, kept)
    phase = (frequency[:, None] * np.arange(length)[None, :]) % length
    angle = 2.0 * np.pi / length * phase
    return np.cos(angle) * length**-0.5, np.sin(angle) * length**-0.5


def by_half(table):
    re, im = table
    rows = [part[h * HALF : (h + 1) * HALF] for h in (0, 1) for part in (re, im)]
    return np.concatenate(rows, axis=0)


def forward_y_table(ny):
    cos, sin = np_table(KY, ny)
    from_re = by_half((cos, -sin))
    from_im = by_half((sin, cos))
    return np.stack([from_re, from_im])


def inverse_y_table(ny):
    cos, sin = np_table(KY, ny)
    to_re = by_half((cos, -sin)).T
    to_im = by_half((sin, cos)).T
    return np.stack([to_re, to_im])


def x_waves(kx, position, nx):
    frequency = jnp.where(kx < KX // 2, kx, nx - KX + kx)
    phase = frequency * position % nx
    angle = 2.0 * math.pi / nx * phase.astype(F32)
    return jnp.cos(angle) * nx**-0.5, jnp.sin(angle) * nx**-0.5


def x_position(row, local, chip, core):
    own = row < local
    place = jnp.where(own, core * local + row, (1 - core) * local + row - local)
    return chip * 2 * local + place


def forward_x_rows(local, nx, chip, core):
    shape = (2 * KX, 2 * local * CHUNK)
    b = lax.broadcasted_iota(jnp.int32, shape, 0)
    q = lax.broadcasted_iota(jnp.int32, shape, 1)
    cos, sin = x_waves(b // 2, x_position(q // CHUNK, local, chip, core), nx)
    to, of = b % 2, q // HALF % 2
    return jnp.where(to == of, cos, jnp.where(to == 0, sin, -sin))


def inverse_x_rows(local, nx, chip, core):
    shape = (4 * local, KX * CHUNK)
    b = lax.broadcasted_iota(jnp.int32, shape, 0)
    q = lax.broadcasted_iota(jnp.int32, shape, 1)
    cos, sin = x_waves(q // CHUNK, x_position(b // 2, local, chip, core), nx)
    to, of = b % 2, q // HALF % 2
    return jnp.where(to == of, cos, jnp.where(to == 0, -sin, sin))


def spread(rows_ref, full_ref):
    count, width = rows_ref.shape
    ky = lax.broadcasted_iota(jnp.int32, (HALF, width), 0)
    column = jnp.bitwise_and(lax.broadcasted_iota(jnp.int32, (HALF, width), 1), HALF - 1)
    keep = ky == column

    def one(b, carry):
        row = jnp.broadcast_to(rows_ref[pl.ds(b, 1), :], (HALF, width))
        at = pl.multiple_of(b * HALF, HALF)
        full_ref[pl.ds(at, HALF), :] = jnp.where(keep, row, 0.0).astype(BF16)
        return carry

    lax.fori_loop(0, count, one, 0)


def spectral_kernel(
    chips,
    field_ref,
    weight_ref,
    fy_ref,
    fx_ref,
    gx_ref,
    out_ref,
    fbuf,
    wbuf,
    fbig,
    gbig,
    ybuf,
    yfrom,
    parts,
    near,
    relay,
    final,
    sums,
    modes,
    zsend,
    zfrom,
    field_sem,
    weight_sem,
    ssem,
    rsem,
):
    local = fbuf.shape[0]
    me = lax.axis_index("space")
    chip, core = me // 2, lax.rem(me, 2)
    sigma = 1 - 2 * core
    used = [0]
    started = []

    def at(step):
        return lax.rem(chip + sigma * step + 2 * chips, chips)

    def copy(src, dst, device):
        k = used[0]
        used[0] += 1
        made = pltpu.make_async_remote_copy(
            src_ref=src,
            dst_ref=dst,
            send_sem=ssem.at[k],
            recv_sem=rsem.at[k],
            device_id={"space": device},
            device_id_type=MESH,
        )
        started.append(made)
        return made

    def to_chip(src, dst, step):
        return copy(src, dst, 2 * at(step) + core)

    loads = []
    for x in range(local):
        load = pltpu.make_async_copy(field_ref.at[:, x], fbuf.at[x], field_sem.at[x])
        load.start()
        loads.append(load)
    weights = pltpu.make_async_copy(weight_ref, wbuf, weight_sem)
    weights.start()

    barrier = pltpu.get_barrier_semaphore()
    for step in (1, -1, 2, -2, 4, -4, 8, -8):
        pl.semaphore_signal(
            barrier, 1, device_id={"space": 2 * at(step) + core}, device_id_type=MESH
        )
    partner = 2 * chip + 1 - core
    pl.semaphore_signal(barrier, 1, device_id={"space": partner}, device_id_type=MESH)

    spread(fx_ref, fbig)

    for x in range(local):
        loads[x].wait()
        rows = jnp.dot(fy_ref[0], fbuf[x, 0], preferred_element_type=F32)
        rows += jnp.dot(fy_ref[1], fbuf[x, 1], preferred_element_type=F32)
        rows = rows.astype(BF16)
        ybuf[0, x] = rows[:CHUNK]
        ybuf[1, x] = rows[CHUNK:]

    pl.semaphore_wait(barrier, 9)
    swap = copy(ybuf.at[1 - core], yfrom, partner)
    swap.start()
    width = ybuf.shape[-1]
    half = local * CHUNK
    own_rows = ybuf[core].reshape(half, width)
    swap.wait_recv()
    other_rows = yfrom[...].reshape(half, width)
    block = 8 * CHUNK
    for b in range(KX * CHUNK // block):
        here = pl.ds(b * block, block)
        part = jnp.dot(fbig[here, :half], own_rows, preferred_element_type=F32)
        part += jnp.dot(fbig[here, half:], other_rows, preferred_element_type=F32)
        parts[b * 8 : (b + 1) * 8] = part.astype(BF16).reshape(8, CHUNK, width)

    arrivals = {}
    for t, step in enumerate(FAR):
        for o, off in enumerate(NEAR):
            sent = to_chip(parts.at[at(4 * step - off)], near.at[o, t], -off)
            sent.start()
            arrivals[o, t] = sent

    spread(gx_ref, gbig)

    def near_sum(t):
        total = parts[at(4 * FAR[t])].astype(F32)
        for o in range(len(NEAR)):
            arrivals[o, t].wait_recv()
            total += near[o, t].astype(F32)
        return total

    def pass_on(t, total, dst, step):
        sums[t] = total.astype(BF16)
        sent = to_chip(sums.at[t], dst, step)
        sent.start()
        return sent

    relay_4 = pass_on(0, near_sum(0), relay.at[0], -8)
    relay_3 = pass_on(1, near_sum(1), relay.at[1], 4)
    relay_m3 = pass_on(2, near_sum(2), relay.at[2], -4)
    total_2, total_m2 = near_sum(3), near_sum(4)
    final_1 = pass_on(5, near_sum(5), final.at[2], 4)
    final_m1 = pass_on(6, near_sum(6), final.at[3], -4)
    mine = near_sum(7)
    relay_3.wait_recv()
    final_2 = pass_on(3, total_2 + relay[1].astype(F32), final.at[0], 8)
    relay_m3.wait_recv()
    total_m2 += relay[2].astype(F32)
    relay_4.wait_recv()
    final_m2 = pass_on(4, total_m2 + relay[0].astype(F32), final.at[1], -8)
    final_1.wait_recv()
    mine += final[2].astype(F32)
    final_m1.wait_recv()
    mine += final[3].astype(F32)
    weights.wait()
    final_2.wait_recv()
    mine += final[0].astype(F32)
    final_m2.wait_recv()
    mine += final[1].astype(F32)

    ky = jnp.bitwise_and(lax.broadcasted_iota(jnp.int32, mine.shape, 0), HALF - 1)
    by_re = jnp.zeros(mine.shape, F32)
    by_im = jnp.zeros(mine.shape, F32)
    for m in range(HALF):
        row = jnp.where(ky == m, mine, 0.0).astype(BF16)
        by_re += jnp.dot(row, wbuf[m, 0], preferred_element_type=F32)
        by_im += jnp.dot(row, wbuf[m, 1], preferred_element_type=F32)
    mixed_re = by_re[:HALF] - by_im[HALF:]
    mixed_im = by_im[:HALF] + by_re[HALF:]
    modes[chip] = jnp.concatenate([mixed_re, mixed_im], axis=0).astype(BF16)

    gathered = []

    def share(slot, step):
        sent = to_chip(modes.at[slot], modes.at[slot], step)
        sent.start()
        return sent

    def serve(slot):
        for off in NEAR:
            gathered.append(share(slot, off))

    go_2 = share(chip, 8)
    go_m2 = share(chip, -8)
    go_1 = share(chip, 4)
    go_m1 = share(chip, -4)
    serve(chip)

    go_1.wait_recv()
    serve(at(-4))
    go_m1.wait_recv()
    serve(at(4))
    go_2.wait_recv()
    go_4 = share(at(-8), 8)
    go_3 = share(at(-8), 4)
    serve(at(-8))
    go_m2.wait_recv()
    go_m3 = share(at(8), -4)
    serve(at(8))
    go_3.wait_recv()
    serve(at(-12))
    go_m3.wait_recv()
    serve(at(12))
    go_4.wait_recv()
    serve(at(-16))
    for sent in gathered:
        sent.wait_recv()

    all_modes = modes[...].reshape(KX * CHUNK, width)
    other = jnp.dot(gbig[half:, :], all_modes, preferred_element_type=F32)
    zsend[...] = other.astype(BF16).reshape(local, CHUNK, width)
    back = copy(zsend, zfrom, partner)
    back.start()
    own = jnp.dot(gbig[:half, :], all_modes, preferred_element_type=F32)
    out_ref[:, core] = own.astype(BF16).reshape(local, CHUNK, width)
    back.wait_recv()
    out_ref[:, 1 - core] = zfrom[...]
    for sent in started:
        sent.wait_send()


def finish_kernel(field_ref, z_ref, skip_ref, gy_ref, out_ref):
    z = z_ref[0].reshape(2 * CHUNK, z_ref.shape[-1])
    z = jnp.concatenate([z, z], axis=0)
    skip = skip_ref[...]
    for part in (0, 1):
        spectral = jnp.dot(gy_ref[part], z, preferred_element_type=F32)
        total = spectral + jnp.dot(field_ref[part, 0], skip, preferred_element_type=F32)
        out_ref[part, 0] = total.astype(BF16)


def shards(field, spectral_weight, skip_weight):
    devices = lax.axis_size("space")
    chips = devices // 2
    _, local, ny, width = field.shape
    nx = local * devices
    assert spectral_weight.shape[0] == HALF and chips == KX
    me = lax.axis_index("space")
    chip, core = me // 2, lax.rem(me, 2)
    fy = jnp.asarray(forward_y_table(ny), BF16)
    gy = inverse_y_table(ny).astype(np.float32)
    gy_high = np.asarray(gy.astype(jnp.bfloat16), np.float32)
    gy = jnp.asarray(np.concatenate([gy_high, gy - gy_high], axis=2), BF16)
    fx = forward_x_rows(local, nx, chip, core)
    gx = inverse_x_rows(local, nx, chip, core)
    vmem = pl.BlockSpec(memory_space=pltpu.VMEM)
    hbm = pl.BlockSpec(memory_space=pl.ANY)
    copies = 2 + 2 * (len(NEAR) * len(FAR) + len(FAR) - 1)
    z = pl.pallas_call(
        functools.partial(spectral_kernel, chips),
        out_shape=jax.ShapeDtypeStruct((local, 2, CHUNK, width), BF16),
        in_specs=[hbm, hbm, vmem, vmem, vmem],
        out_specs=vmem,
        scratch_shapes=[
            pltpu.VMEM((local, 2, ny, width), BF16),
            pltpu.VMEM(spectral_weight.shape, BF16),
            pltpu.VMEM((KX * CHUNK, 2 * local * CHUNK), BF16),
            pltpu.VMEM((2 * local * CHUNK, KX * CHUNK), BF16),
            pltpu.VMEM((2, local, CHUNK, width), BF16),
            pltpu.VMEM((local, CHUNK, width), BF16),
            pltpu.VMEM((KX, CHUNK, width), BF16),
            pltpu.VMEM((len(NEAR), len(FAR), CHUNK, width), BF16),
            pltpu.VMEM((3, CHUNK, width), BF16),
            pltpu.VMEM((4, CHUNK, width), BF16),
            pltpu.VMEM((len(FAR), CHUNK, width), BF16),
            pltpu.VMEM((KX, CHUNK, width), BF16),
            pltpu.VMEM((local, CHUNK, width), BF16),
            pltpu.VMEM((local, CHUNK, width), BF16),
            pltpu.SemaphoreType.DMA((local,)),
            pltpu.SemaphoreType.DMA,
            pltpu.SemaphoreType.DMA((copies,)),
            pltpu.SemaphoreType.DMA((copies,)),
        ],
        name="spectral",
        compiler_params=pltpu.CompilerParams(collective_id=1, has_side_effects=True),
    )(field, spectral_weight, fy, fx, gx)
    rows = pl.BlockSpec((2, 1, ny, width), lambda x: (0, x, 0, 0))
    return pl.pallas_call(
        finish_kernel,
        grid=(local,),
        out_shape=jax.ShapeDtypeStruct(field.shape, BF16),
        in_specs=[
            rows,
            pl.BlockSpec((1, 2, CHUNK, width), lambda x: (x, 0, 0, 0)),
            pl.BlockSpec((width, width), lambda x: (0, 0)),
            pl.BlockSpec(gy.shape, lambda x: (0, 0, 0)),
        ],
        out_specs=rows,
        name="finish",
    )(field, z, skip_weight, gy)


def solution(mesh):
    return jax.shard_map(
        shards,
        mesh=mesh,
        in_specs=(P("group", "space", None, None), P("space", None, None, None), P()),
        out_specs=P("group", "space", None, None),
        check_vma=False,
    )
```

```python
import functools

import jax
import jax.numpy as jnp
import numpy as np
from jax import lax
from jax.experimental import pallas as pl
from jax.experimental.pallas import tpu as pltpu
from jax.sharding import PartitionSpec as P

KX = 32
KY = 32
HALF = KY // 2
CHUNK = 2 * HALF
ROWS = 2
FIRST_VMEM = 26 << 20
LAST_VMEM = 14 << 20
MESH = pl.DeviceIdType.MESH
F32 = jnp.float32
BF16 = jnp.bfloat16
NEAR = (-2, -1, 1)
FAR = (4, 3, -3, 2, -2, 1, -1, 0)


def frequency_of(index, length, kept):
    return np.where(index < kept // 2, index, length - kept + index)


def np_table(kept, length):
    frequency = frequency_of(np.arange(kept), length, kept)
    phase = (frequency[:, None] * np.arange(length)[None, :]) % length
    angle = 2.0 * np.pi / length * phase
    return np.cos(angle) * length**-0.5, np.sin(angle) * length**-0.5


def by_half(table):
    re, im = table
    rows = [part[h * HALF : (h + 1) * HALF] for h in (0, 1) for part in (re, im)]
    return np.concatenate(rows, axis=0)


def forward_y_table(ny):
    cos, sin = np_table(KY, ny)
    from_re = by_half((cos, -sin))
    from_im = by_half((sin, cos))
    return np.stack([from_re, from_im])


def inverse_y_table(ny):
    cos, sin = np_table(KY, ny)
    to_re = by_half((cos, -sin)).T
    to_im = by_half((sin, cos)).T
    return np.stack([to_re, to_im])


def x_tables(local, devices):
    nx = local * devices
    cos, sin = np_table(KX, nx)
    tables = np.zeros((devices, 2 * KX + 4 * local, 2 * KX))
    for device in range(devices):
        chip, core = divmod(device, 2)
        rows = [np.arange(local) + (2 * chip + side) * local for side in (core, 1 - core)]
        rows = np.concatenate(rows)
        c, s = cos[:, rows], sin[:, rows]
        forward = np.stack([np.stack([c, s], -1), np.stack([-s, c], -1)], 1)
        forward = forward.reshape(2 * KX, 4 * local)
        tables[device, : 2 * KX, : 4 * local] = forward
        tables[device, 2 * KX :] = forward.T
    return tables


def spread(table, rows_ref, full_ref):
    count, width = rows_ref.shape
    shape = (table.shape[1], width)
    one_hot = lax.broadcasted_iota(jnp.int32, shape, 0) == lax.shift_right_logical(
        lax.broadcasted_iota(jnp.int32, shape, 1), HALF.bit_length() - 1
    )
    one_hot = jnp.where(one_hot, 1.0, 0.0).astype(BF16)
    rows_ref[...] = jnp.dot(table, one_hot, preferred_element_type=F32)
    ky = lax.broadcasted_iota(jnp.int32, (HALF, width), 0)
    column = jnp.bitwise_and(lax.broadcasted_iota(jnp.int32, (HALF, width), 1), HALF - 1)
    keep = ky == column

    def one(b, carry):
        row = jnp.broadcast_to(rows_ref[pl.ds(b, 1), :], (HALF, width))
        at = pl.multiple_of(b * HALF, HALF)
        full_ref[pl.ds(at, HALF), :] = jnp.where(keep, row, 0.0).astype(BF16)
        return carry

    lax.fori_loop(0, count, one, 0, unroll=4)


def spectral_kernel(
    chips,
    field_ref,
    weight_ref,
    skip_hbm,
    fy_hbm,
    table_ref,
    out_ref,
    skipped_ref,
    fbuf,
    wbuf,
    skip_ref,
    fy_ref,
    tbuf,
    frows,
    grows,
    fbig,
    gbig,
    ybuf,
    yfrom,
    parts,
    near,
    relay,
    final,
    sums,
    modes,
    zsend,
    zfrom,
    field_sem,
    weight_sem,
    table_sem,
    fy_sem,
    skip_sem,
    ssem,
    rsem,
    far_sem,
):
    local = fbuf.shape[0]
    me = lax.axis_index("space")
    chip, core = me // 2, lax.rem(me, 2)
    sigma = 1 - 2 * core
    used = [0]
    started = []

    def at(step):
        return lax.rem(chip + sigma * step + 2 * chips, chips)

    def copy(src, dst, device):
        k = used[0]
        used[0] += 1
        made = pltpu.make_async_remote_copy(
            src_ref=src,
            dst_ref=dst,
            send_sem=ssem.at[k],
            recv_sem=rsem.at[k],
            device_id={"space": device},
            device_id_type=MESH,
        )
        started.append(made)
        return made

    def to_chip(src, dst, step):
        return copy(src, dst, 2 * at(step) + core)

    table = pltpu.make_async_copy(table_ref.at[me], tbuf, table_sem)
    table.start()
    waves = pltpu.make_async_copy(fy_hbm, fy_ref, fy_sem)
    waves.start()
    loads = []
    for x in range(local):
        load = pltpu.make_async_copy(field_ref.at[:, x], fbuf.at[x], field_sem.at[x])
        load.start()
        loads.append(load)
    weights = pltpu.make_async_copy(weight_ref, wbuf, weight_sem)
    weights.start()
    skip = pltpu.make_async_copy(skip_hbm, skip_ref, skip_sem)
    skip.start()

    barrier = pltpu.get_barrier_semaphore()
    for step in (4, -4, 2, -2, 1, -1):
        pl.semaphore_signal(
            barrier, 1, device_id={"space": 2 * at(step) + core}, device_id_type=MESH
        )
    partner = 2 * chip + 1 - core
    pl.semaphore_signal(barrier, 1, device_id={"space": partner}, device_id_type=MESH)

    table.wait()
    spread(tbuf[: 2 * KX], frows, fbig)

    waves.wait()
    for x in range(local):
        loads[x].wait()
        rows = jnp.dot(fy_ref[0], fbuf[x, 0], preferred_element_type=F32)
        rows += jnp.dot(fy_ref[1], fbuf[x, 1], preferred_element_type=F32)
        rows = rows.astype(BF16)
        ybuf[0, x] = rows[:CHUNK]
        ybuf[1, x] = rows[CHUNK:]

    pl.semaphore_wait(barrier, 7)
    for step in (4, -4):
        pl.semaphore_signal(
            far_sem, 1, device_id={"space": 2 * at(step) + core}, device_id_type=MESH
        )
    swap = copy(ybuf.at[1 - core], yfrom, partner)
    swap.start()
    width = ybuf.shape[-1]
    half = local * CHUNK
    own_rows = ybuf[core].reshape(half, width)
    swap.wait_recv()
    other_rows = yfrom[...].reshape(half, width)
    block = 8 * CHUNK
    for b in range(KX * CHUNK // block):
        here = pl.ds(b * block, block)
        part = jnp.dot(fbig[here, :half], own_rows, preferred_element_type=F32)
        part += jnp.dot(fbig[here, half:], other_rows, preferred_element_type=F32)
        parts[b * 8 : (b + 1) * 8] = part.astype(BF16).reshape(8, CHUNK, width)

    arrivals = {}
    for t, step in enumerate(FAR):
        for o, off in enumerate(NEAR):
            sent = to_chip(parts.at[at(4 * step - off)], near.at[o, t], -off)
            sent.start()
            arrivals[o, t] = sent

    spread(tbuf[2 * KX :], grows, gbig)

    def near_sum(t):
        total = parts[at(4 * FAR[t])].astype(F32)
        for o in range(len(NEAR)):
            arrivals[o, t].wait_recv()
            total += near[o, t].astype(F32)
        return total

    def pass_on(t, total, dst, step):
        sums[t] = total.astype(BF16)
        sent = to_chip(sums.at[t], dst, step)
        sent.start()
        return sent

    pl.semaphore_wait(far_sem, 2)
    relay_4 = pass_on(0, near_sum(0), relay.at[0], -8)
    relay_3 = pass_on(1, near_sum(1), relay.at[1], 4)
    relay_m3 = pass_on(2, near_sum(2), relay.at[2], -4)
    total_2, total_m2 = near_sum(3), near_sum(4)
    final_1 = pass_on(5, near_sum(5), final.at[2], 4)
    final_m1 = pass_on(6, near_sum(6), final.at[3], -4)
    mine = near_sum(7)

    skip.wait()

    def skip_rows(n, carry):
        x, part = n // 2, lax.rem(n, 2)
        skipped_ref[x, part] = jnp.dot(
            fbuf[x, part], skip_ref[...], preferred_element_type=F32
        )
        return carry

    lax.fori_loop(0, 2 * local, skip_rows, 0)
    relay_3.wait_recv()
    final_2 = pass_on(3, total_2 + relay[1].astype(F32), final.at[0], 8)
    relay_m3.wait_recv()
    total_m2 += relay[2].astype(F32)
    relay_4.wait_recv()
    final_m2 = pass_on(4, total_m2 + relay[0].astype(F32), final.at[1], -8)
    final_1.wait_recv()
    mine += final[2].astype(F32)
    final_m1.wait_recv()
    mine += final[3].astype(F32)
    weights.wait()
    final_2.wait_recv()
    mine += final[0].astype(F32)
    final_m2.wait_recv()
    mine += final[1].astype(F32)

    ky = jnp.bitwise_and(lax.broadcasted_iota(jnp.int32, mine.shape, 0), HALF - 1)
    by_re = jnp.zeros(mine.shape, F32)
    by_im = jnp.zeros(mine.shape, F32)
    for m in range(HALF):
        row = jnp.where(ky == m, mine, 0.0).astype(BF16)
        by_re += jnp.dot(row, wbuf[m, 0], preferred_element_type=F32)
        by_im += jnp.dot(row, wbuf[m, 1], preferred_element_type=F32)
    mixed_re = by_re[:HALF] - by_im[HALF:]
    mixed_im = by_im[:HALF] + by_re[HALF:]
    modes[chip] = jnp.concatenate([mixed_re, mixed_im], axis=0).astype(BF16)

    gathered = []

    def share(slot, step):
        sent = to_chip(modes.at[slot], modes.at[slot], step)
        sent.start()
        return sent

    def serve(slot):
        for off in NEAR:
            gathered.append(share(slot, off))

    go_2 = share(chip, 8)
    go_m2 = share(chip, -8)
    go_1 = share(chip, 4)
    go_m1 = share(chip, -4)
    serve(chip)

    go_1.wait_recv()
    serve(at(-4))
    go_m1.wait_recv()
    serve(at(4))
    go_2.wait_recv()
    go_4 = share(at(-8), 8)
    go_3 = share(at(-8), 4)
    serve(at(-8))
    go_m2.wait_recv()
    go_m3 = share(at(8), -4)
    serve(at(8))
    go_3.wait_recv()
    serve(at(-12))
    go_m3.wait_recv()
    serve(at(12))
    go_4.wait_recv()
    serve(at(-16))
    for sent in gathered:
        sent.wait_recv()

    all_modes = modes[...].reshape(KX * CHUNK, width)
    other = jnp.dot(gbig[half:, :], all_modes, preferred_element_type=F32)
    zsend[...] = other.astype(BF16).reshape(local, CHUNK, width)
    back = copy(zsend, zfrom, partner)
    back.start()
    own = jnp.dot(gbig[:half, :], all_modes, preferred_element_type=F32)
    out_ref[:, core] = own.astype(BF16).reshape(local, CHUNK, width)
    back.wait_recv()
    out_ref[:, 1 - core] = zfrom[...]
    for sent in started:
        sent.wait_send()


def finish_kernel(skipped_ref, z_ref, gy_ref, out_ref):
    block = out_ref.shape[1]
    for x in range(block):
        row = pl.program_id(0) * block + x
        z = z_ref[row].reshape(2 * CHUNK, z_ref.shape[-1])
        z = jnp.concatenate([z, z], axis=0)
        for part in (0, 1):
            spectral = jnp.dot(gy_ref[part], z, preferred_element_type=F32)
            out_ref[part, x] = (spectral + skipped_ref[row, part]).astype(BF16)


def shards(field, spectral_weight, skip_weight):
    devices = lax.axis_size("space")
    chips = devices // 2
    _, local, ny, width = field.shape
    assert spectral_weight.shape[0] == HALF and chips == KX
    fy = jnp.asarray(forward_y_table(ny), BF16)
    gy = inverse_y_table(ny).astype(np.float32)
    gy_high = np.asarray(gy.astype(jnp.bfloat16), np.float32)
    gy = jnp.asarray(np.concatenate([gy_high, gy - gy_high], axis=2), BF16)
    tables = jnp.asarray(x_tables(local, devices), BF16)
    vmem = pl.BlockSpec(memory_space=pltpu.VMEM)
    hbm = pl.BlockSpec(memory_space=pltpu.HBM)
    copies = 2 + 2 * (len(NEAR) * len(FAR) + len(FAR) - 1)
    arrays = (field, spectral_weight, skip_weight, fy, tables)
    z, skipped = pl.pallas_call(
        functools.partial(spectral_kernel, chips),
        out_shape=(
            jax.ShapeDtypeStruct((local, 2, CHUNK, width), BF16),
            jax.ShapeDtypeStruct((local, 2, ny, width), F32),
        ),
        in_specs=[hbm] * 5,
        out_specs=(vmem, vmem),
        scratch_shapes=[
            pltpu.VMEM((local, 2, ny, width), BF16),
            pltpu.VMEM(spectral_weight.shape, BF16),
            pltpu.VMEM(skip_weight.shape, BF16),
            pltpu.VMEM(fy.shape, BF16),
            pltpu.VMEM(tables.shape[1:], BF16),
            pltpu.VMEM((2 * KX, 2 * local * CHUNK), F32),
            pltpu.VMEM((4 * local, KX * CHUNK), F32),
            pltpu.VMEM((KX * CHUNK, 2 * local * CHUNK), BF16),
            pltpu.VMEM((2 * local * CHUNK, KX * CHUNK), BF16),
            pltpu.VMEM((2, local, CHUNK, width), BF16),
            pltpu.VMEM((local, CHUNK, width), BF16),
            pltpu.VMEM((KX, CHUNK, width), BF16),
            pltpu.VMEM((len(NEAR), len(FAR), CHUNK, width), BF16),
            pltpu.VMEM((3, CHUNK, width), BF16),
            pltpu.VMEM((4, CHUNK, width), BF16),
            pltpu.VMEM((len(FAR), CHUNK, width), BF16),
            pltpu.VMEM((KX, CHUNK, width), BF16),
            pltpu.VMEM((local, CHUNK, width), BF16),
            pltpu.VMEM((local, CHUNK, width), BF16),
            pltpu.SemaphoreType.DMA((local,)),
            pltpu.SemaphoreType.DMA,
            pltpu.SemaphoreType.DMA,
            pltpu.SemaphoreType.DMA,
            pltpu.SemaphoreType.DMA,
            pltpu.SemaphoreType.DMA((copies,)),
            pltpu.SemaphoreType.DMA((copies,)),
            pltpu.SemaphoreType.REGULAR,
        ],
        name="spectral",
        compiler_params=pltpu.CompilerParams(
            collective_id=1, has_side_effects=True, vmem_limit_bytes=FIRST_VMEM
        ),
    )(*(pltpu.with_memory_space_constraint(array, pltpu.HBM) for array in arrays))
    return pl.pallas_call(
        finish_kernel,
        grid=(local // ROWS,),
        out_shape=jax.ShapeDtypeStruct(field.shape, BF16),
        in_specs=[vmem, vmem, vmem],
        out_specs=pl.BlockSpec((2, ROWS, ny, width), lambda x: (0, x, 0, 0)),
        name="finish",
        compiler_params=pltpu.CompilerParams(vmem_limit_bytes=LAST_VMEM),
    )(skipped, z, gy)


def solution(mesh):
    return jax.shard_map(
        shards,
        mesh=mesh,
        in_specs=(P("group", "space", None, None), P("space", None, None, None), P()),
        out_specs=P("group", "space", None, None),
        check_vma=False,
    )
```

```python
import functools

import jax
import jax.numpy as jnp
import numpy as np
from jax import lax
from jax.experimental import pallas as pl
from jax.experimental.pallas import tpu as pltpu
from jax.sharding import PartitionSpec as P

KX = 32
KY = 32
HALF = KY // 2
CHUNK = 2 * HALF
ROWS = 2
FIRST_VMEM = 26 << 20
LAST_VMEM = 14 << 20
MESH = pl.DeviceIdType.MESH
F32 = jnp.float32
BF16 = jnp.bfloat16
HUBS = {
    12: (4, 3, 2, -2, 1, -1),
    -12: (-3, -2, 1, -1),
    8: (-2, 1, -1),
    -8: (-2, 1, -1),
    4: (-2, 1, -1),
    -4: (-2, 1, -1),
    0: (-2, 1, -1),
}
NEAR_COPIES = sum(len(offsets) for offsets in HUBS.values())


def frequency_of(index, length, kept):
    return np.where(index < kept // 2, index, length - kept + index)


def np_table(kept, length):
    frequency = frequency_of(np.arange(kept), length, kept)
    phase = (frequency[:, None] * np.arange(length)[None, :]) % length
    angle = 2.0 * np.pi / length * phase
    return np.cos(angle) * length**-0.5, np.sin(angle) * length**-0.5


def by_half(table):
    re, im = table
    rows = [part[h * HALF : (h + 1) * HALF] for h in (0, 1) for part in (re, im)]
    return np.concatenate(rows, axis=0)


def forward_y_table(ny):
    cos, sin = np_table(KY, ny)
    from_re = by_half((cos, -sin))
    from_im = by_half((sin, cos))
    return np.stack([from_re, from_im])


def inverse_y_table(ny):
    cos, sin = np_table(KY, ny)
    to_re = by_half((cos, -sin)).T
    to_im = by_half((sin, cos)).T
    return np.stack([to_re, to_im])


def x_tables(local, devices):
    nx = local * devices
    cos, sin = np_table(KX, nx)
    tables = np.zeros((devices, 2 * KX + 4 * local, 2 * KX))
    for device in range(devices):
        chip, core = divmod(device, 2)
        rows = [np.arange(local) + (2 * chip + side) * local for side in (core, 1 - core)]
        rows = np.concatenate(rows)
        c, s = cos[:, rows], sin[:, rows]
        forward = np.stack([np.stack([c, s], -1), np.stack([-s, c], -1)], 1)
        forward = forward.reshape(2 * KX, 4 * local)
        tables[device, : 2 * KX, : 4 * local] = forward
        tables[device, 2 * KX :] = forward.T
    return tables


def spread(table, rows_ref, full_ref):
    count, width = rows_ref.shape
    shape = (table.shape[1], width)
    one_hot = lax.broadcasted_iota(jnp.int32, shape, 0) == lax.shift_right_logical(
        lax.broadcasted_iota(jnp.int32, shape, 1), HALF.bit_length() - 1
    )
    one_hot = jnp.where(one_hot, 1.0, 0.0).astype(BF16)
    rows_ref[...] = jnp.dot(table, one_hot, preferred_element_type=F32)
    ky = lax.broadcasted_iota(jnp.int32, (HALF, width), 0)
    column = jnp.bitwise_and(lax.broadcasted_iota(jnp.int32, (HALF, width), 1), HALF - 1)
    keep = ky == column

    def one(b, carry):
        row = jnp.broadcast_to(rows_ref[pl.ds(b, 1), :], (HALF, width))
        at = pl.multiple_of(b * HALF, HALF)
        full_ref[pl.ds(at, HALF), :] = jnp.where(keep, row, 0.0).astype(BF16)
        return carry

    lax.fori_loop(0, count, one, 0, unroll=4)


def spectral_kernel(
    chips,
    field_ref,
    weight_ref,
    skip_hbm,
    fy_hbm,
    table_ref,
    out_ref,
    skipped_ref,
    fbuf,
    wbuf,
    skip_ref,
    fy_ref,
    tbuf,
    frows,
    grows,
    fbig,
    gbig,
    ybuf,
    yfrom,
    parts,
    near,
    final,
    sums,
    modes,
    zsend,
    zfrom,
    field_sem,
    weight_sem,
    table_sem,
    fy_sem,
    skip_sem,
    ssem,
    rsem,
    far_sem,
    farther_sem,
):
    local = fbuf.shape[0]
    me = lax.axis_index("space")
    chip, core = me // 2, lax.rem(me, 2)
    sigma = 1 - 2 * core
    used = [0]
    started = []

    def at(step):
        return lax.rem(chip + sigma * step + 2 * chips, chips)

    def copy(src, dst, device):
        k = used[0]
        used[0] += 1
        made = pltpu.make_async_remote_copy(
            src_ref=src,
            dst_ref=dst,
            send_sem=ssem.at[k],
            recv_sem=rsem.at[k],
            device_id={"space": device},
            device_id_type=MESH,
        )
        started.append(made)
        return made

    def to_chip(src, dst, step):
        return copy(src, dst, 2 * at(step) + core)

    table = pltpu.make_async_copy(table_ref.at[me], tbuf, table_sem)
    table.start()
    waves = pltpu.make_async_copy(fy_hbm, fy_ref, fy_sem)
    waves.start()

    def signal_chip(semaphore, step):
        device = {"space": 2 * at(step) + core}
        pl.semaphore_signal(semaphore, 1, device_id=device, device_id_type=MESH)

    loads = []
    for x in range(local):
        load = pltpu.make_async_copy(field_ref.at[:, x], fbuf.at[x], field_sem.at[x])
        load.start()
        loads.append(load)
    weights = pltpu.make_async_copy(weight_ref, wbuf, weight_sem)
    skip = pltpu.make_async_copy(skip_hbm, skip_ref, skip_sem)

    barrier = pltpu.get_barrier_semaphore()
    for step in (4, -4, 3, -3, 2, -2, 1, -1):
        signal_chip(barrier, step)
    partner = 2 * chip + 1 - core
    pl.semaphore_signal(barrier, 1, device_id={"space": partner}, device_id_type=MESH)

    table.wait()
    spread(tbuf[: 2 * KX], frows, fbig)

    waves.wait()
    for x in range(local):
        loads[x].wait()
        rows = jnp.dot(fy_ref[0], fbuf[x, 0], preferred_element_type=F32)
        rows += jnp.dot(fy_ref[1], fbuf[x, 1], preferred_element_type=F32)
        rows = rows.astype(BF16)
        ybuf[0, x] = rows[:CHUNK]
        ybuf[1, x] = rows[CHUNK:]

    weights.start()
    skip.start()
    pl.semaphore_wait(barrier, 9)
    signal_chip(far_sem, 4)
    signal_chip(far_sem, -4)
    swap = copy(ybuf.at[1 - core], yfrom, partner)
    swap.start()
    width = ybuf.shape[-1]
    half = local * CHUNK
    own_rows = ybuf[core].reshape(half, width)
    swap.wait_recv()
    other_rows = yfrom[...].reshape(half, width)
    block = 8 * CHUNK
    for b in range(KX * CHUNK // block):
        here = pl.ds(b * block, block)
        part = jnp.dot(fbig[here, :half], own_rows, preferred_element_type=F32)
        part += jnp.dot(fbig[here, half:], other_rows, preferred_element_type=F32)
        parts[b * 8 : (b + 1) * 8] = part.astype(BF16).reshape(8, CHUNK, width)

    arrivals = {}
    for hub, offsets in HUBS.items():
        for offset in offsets:
            slot = len(arrivals)
            sent = to_chip(parts.at[at(-offset - hub)], near.at[slot], -offset)
            sent.start()
            arrivals[hub, offset] = sent, slot
    pl.semaphore_wait(far_sem, 2)
    signal_chip(farther_sem, 4)
    signal_chip(farther_sem, -4)

    spread(tbuf[2 * KX :], grows, gbig)

    def near_sum(hub):
        total = parts[at(-hub)].astype(F32)
        for offset in HUBS[hub]:
            sent, slot = arrivals[hub, offset]
            sent.wait_recv()
            total += near[slot].astype(F32)
        return total

    pl.semaphore_wait(farther_sem, 2)
    finals = []
    for hub in HUBS:
        if hub == 0:
            continue
        slot = len(finals)
        sums[slot] = near_sum(hub).astype(BF16)
        sent = to_chip(sums.at[slot], final.at[slot], -hub)
        sent.start()
        finals.append(sent)
    mine = near_sum(0)

    skip.wait()

    def skip_rows(n, carry):
        x, part = n // 2, lax.rem(n, 2)
        skipped_ref[x, part] = jnp.dot(
            fbuf[x, part], skip_ref[...], preferred_element_type=F32
        )
        return carry

    lax.fori_loop(0, 2 * local, skip_rows, 0)
    weights.wait()
    for slot in reversed(range(len(finals))):
        finals[slot].wait_recv()
        mine += final[slot].astype(F32)

    ky = jnp.bitwise_and(lax.broadcasted_iota(jnp.int32, mine.shape, 0), HALF - 1)
    by_re = jnp.zeros(mine.shape, F32)
    by_im = jnp.zeros(mine.shape, F32)
    for m in range(HALF):
        row = jnp.where(ky == m, mine, 0.0).astype(BF16)
        by_re += jnp.dot(row, wbuf[m, 0], preferred_element_type=F32)
        by_im += jnp.dot(row, wbuf[m, 1], preferred_element_type=F32)
    mixed_re = by_re[:HALF] - by_im[HALF:]
    mixed_im = by_im[:HALF] + by_re[HALF:]
    modes[chip] = jnp.concatenate([mixed_re, mixed_im], axis=0).astype(BF16)

    gathered = []

    def share(slot, step):
        sent = to_chip(modes.at[slot], modes.at[slot], step)
        sent.start()
        return sent

    shared = {hub: share(chip, hub) for hub in HUBS if hub != 0}
    for hub in reversed(HUBS):
        if hub != 0:
            shared[hub].wait_recv()
        for offset in HUBS[hub]:
            gathered.append(share(at(-hub), offset))
    for sent in gathered:
        sent.wait_recv()

    all_modes = modes[...].reshape(KX * CHUNK, width)
    other = jnp.dot(gbig[half:, :], all_modes, preferred_element_type=F32)
    zsend[...] = other.astype(BF16).reshape(local, CHUNK, width)
    back = copy(zsend, zfrom, partner)
    back.start()
    own = jnp.dot(gbig[:half, :], all_modes, preferred_element_type=F32)
    out_ref[:, core] = own.astype(BF16).reshape(local, CHUNK, width)
    back.wait_recv()
    out_ref[:, 1 - core] = zfrom[...]
    for sent in started:
        sent.wait_send()


def finish_kernel(skipped_ref, z_ref, gy_ref, out_ref):
    block = out_ref.shape[1]
    for x in range(block):
        row = pl.program_id(0) * block + x
        z = z_ref[row].reshape(2 * CHUNK, z_ref.shape[-1])
        z = jnp.concatenate([z, z], axis=0)
        for part in (0, 1):
            spectral = jnp.dot(gy_ref[part], z, preferred_element_type=F32)
            out_ref[part, x] = (spectral + skipped_ref[row, part]).astype(BF16)


def shards(field, spectral_weight, skip_weight):
    devices = lax.axis_size("space")
    chips = devices // 2
    _, local, ny, width = field.shape
    assert spectral_weight.shape[0] == HALF and chips == KX
    fy = jnp.asarray(forward_y_table(ny), BF16)
    gy = inverse_y_table(ny).astype(np.float32)
    gy_high = np.asarray(gy.astype(jnp.bfloat16), np.float32)
    gy = jnp.asarray(np.concatenate([gy_high, gy - gy_high], axis=2), BF16)
    tables = jnp.asarray(x_tables(local, devices), BF16)
    vmem = pl.BlockSpec(memory_space=pltpu.VMEM)
    hbm = pl.BlockSpec(memory_space=pltpu.HBM)
    copies = 2 + 2 * (NEAR_COPIES + len(HUBS) - 1)
    arrays = (field, spectral_weight, skip_weight, fy, tables)
    z, skipped = pl.pallas_call(
        functools.partial(spectral_kernel, chips),
        out_shape=(
            jax.ShapeDtypeStruct((local, 2, CHUNK, width), BF16),
            jax.ShapeDtypeStruct((local, 2, ny, width), F32),
        ),
        in_specs=[hbm] * 5,
        out_specs=(vmem, vmem),
        scratch_shapes=[
            pltpu.VMEM((local, 2, ny, width), BF16),
            pltpu.VMEM(spectral_weight.shape, BF16),
            pltpu.VMEM(skip_weight.shape, BF16),
            pltpu.VMEM(fy.shape, BF16),
            pltpu.VMEM(tables.shape[1:], BF16),
            pltpu.VMEM((2 * KX, 2 * local * CHUNK), F32),
            pltpu.VMEM((4 * local, KX * CHUNK), F32),
            pltpu.VMEM((KX * CHUNK, 2 * local * CHUNK), BF16),
            pltpu.VMEM((2 * local * CHUNK, KX * CHUNK), BF16),
            pltpu.VMEM((2, local, CHUNK, width), BF16),
            pltpu.VMEM((local, CHUNK, width), BF16),
            pltpu.VMEM((KX, CHUNK, width), BF16),
            pltpu.VMEM((NEAR_COPIES, CHUNK, width), BF16),
            pltpu.VMEM((len(HUBS) - 1, CHUNK, width), BF16),
            pltpu.VMEM((len(HUBS) - 1, CHUNK, width), BF16),
            pltpu.VMEM((KX, CHUNK, width), BF16),
            pltpu.VMEM((local, CHUNK, width), BF16),
            pltpu.VMEM((local, CHUNK, width), BF16),
            pltpu.SemaphoreType.DMA((local,)),
            pltpu.SemaphoreType.DMA,
            pltpu.SemaphoreType.DMA,
            pltpu.SemaphoreType.DMA,
            pltpu.SemaphoreType.DMA,
            pltpu.SemaphoreType.DMA((copies,)),
            pltpu.SemaphoreType.DMA((copies,)),
            pltpu.SemaphoreType.REGULAR,
            pltpu.SemaphoreType.REGULAR,
        ],
        name="spectral",
        compiler_params=pltpu.CompilerParams(
            collective_id=1, has_side_effects=True, vmem_limit_bytes=FIRST_VMEM
        ),
    )(*(pltpu.with_memory_space_constraint(array, pltpu.HBM) for array in arrays))
    return pl.pallas_call(
        finish_kernel,
        grid=(local // ROWS,),
        out_shape=jax.ShapeDtypeStruct(field.shape, BF16),
        in_specs=[vmem, vmem, vmem],
        out_specs=pl.BlockSpec((2, ROWS, ny, width), lambda x: (0, x, 0, 0)),
        name="finish",
        compiler_params=pltpu.CompilerParams(vmem_limit_bytes=LAST_VMEM),
    )(skipped, z, gy)


def solution(mesh):
    return jax.shard_map(
        shards,
        mesh=mesh,
        in_specs=(P("group", "space", None, None), P("space", None, None, None), P()),
        out_specs=P("group", "space", None, None),
        check_vma=False,
    )
```
